32 devices in a mesh: slab: 8 (over z, x), rhs: 4 (over y, core).
Axes of the slice: x: 2, y: 2, z: 4, core: 2. Of those that a mesh axis runs over, the one named last changes fastest.
Arguments:
- targets: float32 [8, 128, 256], P('rhs', 'slab'), may hold values from -60 to 60
- counts: int32 [128], P('slab'), may hold values from 1 to 256, 20480 in all
- cell_rows: int32 [128, 256], P('slab'), may hold values from 0 to 255
- cell_cols: int32 [128, 256], P('slab'), may hold values from 0 to 127
- fractions: float32 [2, 128, 256], P(None, 'slab'), may hold values from 0 to 1
- spectrum: float32 [2048, 2048], P(None, ('slab', 'rhs')), may hold values from 0.25 to 4, as said below
- noise_var: float32 [1], replicated, may hold values from 0.1 to 1
Outputs:
- solution: float32 [8, 128, 256], P('rhs', 'slab')
- residual: float32 [8, 128, 256], P('rhs', 'slab')
The draws below stay inside these ranges and needn't reach their ends.
Inputs may be any that keep to these rules, and one draw needn't show every extreme that they name: Each tile has 256 slots; tile t holds points in its first counts[t] slots, and the other slots are empty: their entries are ignored and their outputs are zero. Even in frequency: spectrum[a, b] = spectrum[(2048 - a) % 2048, (2048 - b) % 2048].
All inputs are finite; a program needn't handle non-finite values. No bound on the sum of `counts` on one device may be relied on, other than what follows from the above.
Results may differ from the reference program's by a relative error of at most 0.0002.
Values sent between devices are 32-bit elements; how exact they have to be, the bound alone decides.
A program may use at most 128 MiB of HBM per device.

```python
import math
import jax
import jax.numpy as jnp
import numpy as np
from jax import lax

G = 2048
TC = 128
CAP = 256
RHS = 8
ITERS = 2
ROWS_DEV = 256
TILES = 16
TILES_ALL = 128


def draw_targets(key, part):
    position = jnp.arange(TILES_ALL, dtype=jnp.float32) / TILES_ALL
    growth = jnp.exp(jnp.log(3.0) * position)[None, :, None]
    values = jax.random.normal(key, (RHS, TILES_ALL, CAP), jnp.float32) * growth
    return jnp.clip(values, -60.0, 60.0)


def draw_spectrum(key, part):
    values = jnp.exp(jax.random.uniform(key, (G, G), jnp.float32, math.log(0.25), math.log(4.0)))
    mirrored = jnp.roll(jnp.flip(values, (0, 1)), 1, (0, 1))
    return jnp.clip(0.5 * (values + mirrored), 0.25, 4.0)


def plant(array, stream_key, low, top_value):
    longest = array.shape.index(max(array.shape))
    spots = []
    for shift in (0, 1):
        where = [jax.random.randint(jax.random.fold_in(stream_key, axis), (), 0, length) for axis, length in enumerate(array.shape)]
        where[longest] = (where[longest] + shift) % array.shape[longest]
        spots.append(tuple(where))
    return array.at[spots[0]].set(low).at[spots[1]].set(top_value)


def levels(own_key, dims, pieces, low, top_value):
    loudness, own = 1.0, jax.random.fold_in(own_key, 6)
    for dim, blocks in pieces:
        steps = jnp.exp(jax.random.uniform(jax.random.fold_in(own, dim), (blocks,), jnp.float32, low / len(pieces), top_value / len(pieces)))
        loudness = loudness * jnp.repeat(steps, dims[dim] // blocks).reshape([-1 if axis == dim else 1 for axis in range(len(dims))])
    return loudness


def split_up(amount, total, bound, lean):
    portions = [(1 << 20) // math.isqrt(grade ** lean) + 1 for grade in range(2, amount + 1)]
    spare, given = total - bound - (amount - 1), [1] * (amount - 1)
    while spare > 0:
        free = [i for i in range(amount - 1) if given[i] < bound]
        mass, remaining = sum([portions[i] for i in free]), spare
        for i in free:
            more = min(bound - given[i], max(1, remaining * portions[i] // mass), spare)
            given[i] = given[i] + more
            spare = spare - more
    return np.array([bound] + given)


def uneven(stream_key, amount, total, most, slope):
    if amount == 2:
        one = jax.random.randint(stream_key, (), max(1, total - most), min(most, total - 1) + 1)
        return jnp.stack([one, total - one])
    sizes = jnp.asarray(split_up(amount, total, most, slope), jnp.int32)
    twos = (amount - 1) // 2
    giver, sink = sizes[1:1 + 2 * twos:2], sizes[2:2 + 2 * twos:2]
    slack = jnp.minimum(giver - 1, most - sink)
    moved = jax.random.randint(jax.random.fold_in(stream_key, 1), (twos,), 0, 1 << 20) % (slack + 1)
    sizes = sizes.at[1:1 + 2 * twos:2].set(giver - moved).at[2:2 + 2 * twos:2].set(sink + moved)
    return sizes[jax.random.permutation(jax.random.fold_in(stream_key, 2), amount)]


def setup_inputs(seed: int = 0) -> dict:
    splits = jax.random.split(jax.random.key(seed), 8)
    return {
        "targets": draw_targets(jax.random.fold_in(splits[7], 71), 0),
        "counts": uneven(splits[1], TILES_ALL, TILES_ALL * CAP * 5 // 8, CAP, 2).astype(jnp.int32),
        "cell_rows": plant(jax.random.randint(splits[2], (TILES_ALL, CAP), 0, ROWS_DEV), jax.random.fold_in(splits[2], 1), 0, ROWS_DEV - 1).astype(jnp.int32),
        "cell_cols": plant(jax.random.randint(splits[3], (TILES_ALL, CAP), 0, TC), jax.random.fold_in(splits[3], 1), 0, TC - 1).astype(jnp.int32),
        "fractions": jnp.clip(1.0 * jax.random.uniform(splits[4], (2, TILES_ALL, CAP), jnp.float32) ** levels(splits[4], (2, TILES_ALL, CAP), ((1, 8),), -0.2, 0.2), 0.0, 1.0),
        "spectrum": draw_spectrum(jax.random.fold_in(splits[7], 71), 0),
        "noise_var": jnp.clip(jnp.exp(jax.random.uniform(splits[6], (1,), jnp.float32, math.log(0.1), math.log(1.0))), 0.1, 1.0),
    }


def cubic_weights(fraction):
    return (((-0.5 * fraction + 1.0) * fraction - 0.5) * fraction,
            (1.5 * fraction - 2.5) * fraction * fraction + 1.0,
            ((-1.5 * fraction + 2.0) * fraction + 0.5) * fraction,
            (0.5 * fraction - 0.5) * fraction * fraction)


def stencil(counts, cell_rows, cell_cols, fractions):
    tile_ids = jnp.arange(TILES_ALL, dtype=jnp.int32)
    row_base = (tile_ids // TILES) * ROWS_DEV
    col_base = (tile_ids % TILES) * TC
    grid_rows = row_base[:, None] + cell_rows
    grid_cols = col_base[:, None] + cell_cols
    slot_ids = jnp.arange(CAP, dtype=jnp.int32)
    live = (slot_ids[None, :] < counts[:, None]).astype(jnp.float32)
    row_weights = cubic_weights(fractions[0])
    col_weights = cubic_weights(fractions[1])
    indices = []
    weights = []
    for row_shift in range(4):
        for col_shift in range(4):
            rows_at = (grid_rows - 1 + row_shift) % G
            cols_at = (grid_cols - 1 + col_shift) % G
            indices.append((rows_at * G + cols_at).astype(jnp.int32).reshape(-1))
            weights.append(row_weights[row_shift] * col_weights[col_shift])
    return live, indices, weights


def kernel_product(grid_field, spectrum):
    return jnp.real(jnp.fft.ifft2(spectrum * jnp.fft.fft2(grid_field))).astype(jnp.float32)


def apply_operator(vector, live, indices, weights, spectrum, noise_var):
    grid_flat = jnp.zeros((RHS, G * G), jnp.float32)
    for flat_index, weight in zip(indices, weights):
        grid_flat = grid_flat.at[:, flat_index].add((weight[None] * vector).reshape(RHS, -1))
    grid = grid_flat.reshape(RHS, G, G)
    smoothed = lax.map(lambda grid_field: kernel_product(grid_field, spectrum), grid)
    smooth_flat = smoothed.reshape(RHS, G * G)
    result = jnp.zeros(vector.shape, jnp.float32)
    for flat_index, weight in zip(indices, weights):
        picked = jnp.take(smooth_flat, flat_index, axis=1).reshape(vector.shape)
        result = result + weight[None] * picked
    return live[None] * result + noise_var[0] * vector


def reference(targets, counts, cell_rows, cell_cols, fractions, spectrum, noise_var):
    live, indices, weights = stencil(counts, cell_rows, cell_cols, fractions)
    residual = live[None] * targets
    direction = residual
    solution = jnp.zeros(residual.shape, jnp.float32)
    norm_now = jnp.sum(residual * residual, axis=(1, 2))
    for repeat in range(ITERS):
        image = apply_operator(direction, live, indices, weights, spectrum, noise_var)
        alpha = norm_now / jnp.sum(direction * image, axis=(1, 2))
        solution = solution + alpha[:, None, None] * direction
        residual = residual - alpha[:, None, None] * image
        if repeat + 1 < ITERS:
            norm_next = jnp.sum(residual * residual, axis=(1, 2))
            direction = residual + (norm_next / norm_now)[:, None, None] * direction
            norm_now = norm_next
    return solution, residual
```

```python
import functools
import math

import jax
import jax.numpy as jnp
import numpy as np
from jax import lax
from jax.experimental import pallas as pl
from jax.experimental.pallas import tpu as pltpu
from jax.sharding import PartitionSpec as P

G = 2048
TC = 128
ITERS = 2
RADIX = 8
LONG = G // RADIX
RIM = 8
WIDE = TC + RIM
NOWHERE = 4 * G
F32 = jnp.float32
BF16 = jnp.bfloat16
NT = (((1,), (1,)), ((), ()))
MESH = pl.DeviceIdType.MESH


def cubic_weights(fraction):
    return (
        ((-0.5 * fraction + 1.0) * fraction - 0.5) * fraction,
        (1.5 * fraction - 2.5) * fraction * fraction + 1.0,
        ((-1.5 * fraction + 2.0) * fraction + 0.5) * fraction,
        (0.5 * fraction - 0.5) * fraction * fraction,
    )


def stencil_table(cell, fraction, extent):
    weights = cubic_weights(fraction)
    position = lax.broadcasted_iota(jnp.int32, (extent, cell.shape[1]), 0)
    table = jnp.zeros((extent, cell.shape[1]), F32)
    for offset in range(4):
        target = cell + (offset - 1)
        target = jnp.where(target < 0, extent - 1, target)
        table = jnp.where(position == target, weights[offset], table)
    return table


def halves(value):
    high = value.astype(BF16)
    return high, (value - high.astype(F32)).astype(BF16)


def dot_pieces(left, right, dims=(((1,), (0,)), ((), ()))):
    dot = functools.partial(lax.dot_general, dimension_numbers=dims, preferred_element_type=F32)
    return dot(left[0], right[0]) + (dot(left[0], right[1]) + dot(left[1], right[0]))


def add(a, b):
    return (a[0] + b[0], a[1] + b[1])


def sub(a, b):
    return (a[0] - b[0], a[1] - b[1])


def quarter(a, sign):
    return (-sign * a[1], sign * a[0])


def dft4(x, sign):
    p, m = add(x[0], x[2]), sub(x[0], x[2])
    q, n = add(x[1], x[3]), quarter(sub(x[1], x[3]), sign)
    return [add(p, q), add(m, n), sub(p, q), sub(m, n)]


def dft8(x, sign):
    even, odd = dft4(x[0::2], sign), dft4(x[1::2], sign)
    r = math.sqrt(0.5)
    a, c = odd[1], odd[3]
    odd = [
        odd[0],
        (r * (a[0] - sign * a[1]), r * (a[1] + sign * a[0])),
        quarter(odd[2], sign),
        (r * (-c[0] - sign * c[1]), r * (-c[1] + sign * c[0])),
    ]
    return [add(e, o) for e, o in zip(even, odd)] + [sub(e, o) for e, o in zip(even, odd)]


class Place:
    def __init__(self):
        self.slabs, self.ranks = lax.axis_size("slab"), lax.axis_size("rhs")
        self.slab, self.rank = lax.axis_index("slab"), lax.axis_index("rhs")
        self.deep = self.slabs // self.ranks
        self.pairs = self.ranks // 2
        self.blocks = self.slabs // 2
        self.classes = self.deep * self.pairs
        self.half = lax.rem(self.rank, 2)
        self.field = lax.div(self.slab, self.deep)
        self.own_class = lax.rem(self.slab, self.deep) * self.pairs + lax.div(self.rank, 2)

    def member(self, field, own_class, half):
        slab = field * self.deep + own_class // self.pairs
        return slab, 2 * (own_class % self.pairs) + half

    def is_me(self, slab, rank):
        return jnp.logical_and(slab == self.slab, rank == self.rank)


def greet(senders, expected):
    barrier = pltpu.get_barrier_semaphore()
    for device, mine in senders:
        if mine is None:
            pl.semaphore_signal(barrier, inc=1, device_id=device, device_id_type=MESH)
        else:

            @pl.when(jnp.logical_not(mine))
            def _(device=device):
                pl.semaphore_signal(barrier, inc=1, device_id=device, device_id_type=MESH)

    pl.semaphore_wait(barrier, expected)


def remote(src, dst, send_sem, recv_sem, device):
    return pltpu.make_async_remote_copy(
        src_ref=src,
        dst_ref=dst,
        send_sem=send_sem,
        recv_sem=recv_sem,
        device_id=device,
        device_id_type=MESH,
    )


def turn_kernel(spectrum, pieces, turned):
    classes, _, kept, _ = pieces.shape
    for d in range(RADIX):
        strided = spectrum[pl.ds(d, LONG, stride=RADIX), :]
        for h in range(LONG // TC):
            turned[h] = strided[h * TC : (h + 1) * TC].T
            for w in range(classes):
                pieces[w, d, :, h * TC : (h + 1) * TC] = turned[h, pl.ds(w, kept, stride=classes), :]


def collect_kernel(with_pieces, *refs):
    if with_pieces:
        stat, targ, pieces, statg, targg, gotp, *sems = refs
    else:
        stat, targ, statg, targg, *sems = refs
    stat_send, stat_recv, targ_send, targ_recv, piece_send, piece_recv, own_sem = sems
    at = Place()
    towards = lax.div(at.slab, at.blocks)
    spot = lax.rem(at.slab, at.blocks)
    base = 2 * lax.div(at.rank, 2)
    parity = lax.rem(at.rank, 2)
    stat_to = [(2 * i + parity, base + towards) for i in range(at.slabs // 2)]
    targ_to = [at.member(at.rank, i, towards) for i in range(at.classes)]
    first = at.half * at.blocks
    stat_from = [(first + b, base + lax.rem(at.slab, 2)) for b in range(at.blocks)]
    targ_from = [(first + b, at.field) for b in range(at.blocks)]
    index = lax.rem(at.slab, at.deep) * at.ranks + at.rank
    peers = []
    if with_pieces:
        for step in range(1, at.slabs):
            other = lax.rem(index + step, at.slabs)
            peers.append((at.field * at.deep + other // at.ranks, other % at.ranks))
    senders = [(d, at.is_me(*d)) for d in stat_from + targ_from] + [(d, None) for d in peers]
    expected = len(peers)
    for device in stat_to + targ_to:
        expected = expected + jnp.where(at.is_me(*device), 0, 1)
    greet(senders, expected)

    for src, dst, goals, send, recv in (
        (stat, statg, stat_to, stat_send, stat_recv),
        (targ, targg, targ_to, targ_send, targ_recv),
    ):
        for i, device in enumerate(goals):
            same = at.is_me(*device)

            @pl.when(jnp.logical_not(same))
            def _(src=src, dst=dst, send=send, recv=recv, i=i, device=device):
                remote(src, dst.at[spot], send.at[i], recv.at[spot], device).start()

            @pl.when(same)
            def _(src=src, dst=dst, recv=recv):
                pltpu.make_async_copy(src, dst.at[spot], recv.at[spot]).start()

    copies = []
    if with_pieces:
        for step, (slab, rank) in enumerate(peers, 1):
            wanted = at.classes * (rank % 2) + (slab % at.deep) * at.pairs + rank // 2
            copy = remote(
                pieces.at[wanted], gotp.at[index], piece_send.at[step], piece_recv.at[step], (slab, rank)
            )
            copy.start()
            copies.append(copy)
        own = pltpu.make_async_copy(
            pieces.at[at.classes * at.half + at.own_class], gotp.at[index], own_sem
        )
        own.start()
        own.wait()

    for src, dst, goals, sources, send, recv in (
        (stat, statg, stat_to, stat_from, stat_send, stat_recv),
        (targ, targg, targ_to, targ_from, targ_send, targ_recv),
    ):
        for i, device in enumerate(goals):

            @pl.when(jnp.logical_not(at.is_me(*device)))
            def _(src=src, dst=dst, send=send, recv=recv, i=i, device=device):
                remote(src, dst.at[spot], send.at[i], recv.at[spot], device).wait_send()

        for b, device in enumerate(sources):
            same = at.is_me(*device)

            @pl.when(jnp.logical_not(same))
            def _(src=src, dst=dst, send=send, recv=recv, b=b, device=device):
                remote(src, dst.at[b], send.at[0], recv.at[b], device).wait_recv()

            @pl.when(same)
            def _(src=src, dst=dst, recv=recv, b=b):
                pltpu.make_async_copy(src, dst.at[b], recv.at[b]).wait()

    for copy in copies:
        copy.wait()


def pair_kernel(main, rim, got_main, got_rim, send_sems, recv_sems):
    at = Place()
    partner = (at.slab, at.rank + 1 - 2 * at.half)
    greet([(partner, None)], 1)
    copies = [
        remote(main, got_main, send_sems.at[0], recv_sems.at[0], partner),
        remote(rim, got_rim, send_sems.at[1], recv_sems.at[1], partner),
    ]
    for copy in copies:
        copy.start()
    for copy in copies:
        copy.wait()


def spread_kernel(
    stat, vec, phases, tab_own, tab_oth, own, own_rim, oth, oth_rim, field, rims
):
    blocks, _, tiles, _ = stat.shape
    _, _, folds, _, rows = field.shape
    ext = rows + RIM
    long = tab_own.shape[1]
    half = tab_own.shape[0] // 2
    span = long // TC
    radix = folds // span

    def clear(b, carry):
        field[b] = jnp.zeros(field.shape[1:], F32)
        rims[b] = jnp.zeros(rims.shape[1:], F32)
        return carry

    lax.fori_loop(0, blocks, clear, 0)

    def one_tile(i, carry):
        b, t = lax.div(i, tiles), lax.rem(i, tiles)
        here = lax.rem(t, folds)
        after, before = lax.rem(t + 1, folds), lax.rem(t + folds - 1, folds)
        slot = [stat[b, j, pl.ds(t, 1), :] for j in range(4)]
        row_tab = stencil_table(slot[0].astype(jnp.int32), slot[2], ext)
        col_tab = stencil_table(slot[1].astype(jnp.int32), slot[3], WIDE)
        v0, v1 = vec[b, 0, pl.ds(t, 1), :], vec[b, 1, pl.ds(t, 1), :]
        part = lax.div(t, span)
        pr, pi = phases[0, part], phases[1, part]
        weighted = jnp.concatenate(
            [col_tab * (v0 * pr - v1 * pi), col_tab * (v0 * pi + v1 * pr)], axis=0
        )
        piece = dot_pieces(halves(weighted), halves(row_tab), NT)
        wr, wi = phases[0, 1], phases[1, 1]
        leave = lax.rem(t + 1, span) == 0
        enter = lax.rem(t, span) == 0
        ar, ai = jnp.where(leave, wr, 1.0), jnp.where(leave, wi, 0.0)
        br, bi = jnp.where(enter, wr, 1.0), jnp.where(enter, -wi, 0.0)
        re, im = piece[TC:WIDE], piece[WIDE + TC :]
        low = lax.broadcasted_iota(jnp.int32, (RIM, ext), 0) < RIM // 2
        ahead = (re * ar - im * ai, re * ai + im * ar)
        behind = (re * br - im * bi, re * bi + im * br)
        for k in range(2):
            block = piece[k * WIDE : k * WIDE + TC]
            field[b, k, here] = field[b, k, here] + block[:, :rows]
            rims[b, k, here] = rims[b, k, here] + block[:, rows:]
            edge = jnp.where(low, ahead[k], 0.0)
            field[b, k, after, :RIM] = field[b, k, after, :RIM] + edge[:, :rows]
            rims[b, k, after, :RIM] = rims[b, k, after, :RIM] + edge[:, rows:]
            edge = jnp.where(low, 0.0, behind[k])
            field[b, k, before, TC - RIM :] = field[b, k, before, TC - RIM :] + edge[:, :rows]
            rims[b, k, before, TC - RIM :] = rims[b, k, before, TC - RIM :] + edge[:, rows:]
        return carry

    lax.fori_loop(0, blocks * tiles, one_tile, 0)
    first = lax.broadcasted_iota(jnp.int32, (TC, RIM), 1) < RIM // 2

    def merge(i, carry):
        k, ft = lax.div(i, folds), lax.rem(i, folds)
        for b in range(blocks):
            rim = rims[b, k, ft]
            if b + 1 < blocks:
                up = field[b + 1, k, ft, :, :RIM]
                field[b + 1, k, ft, :, :RIM] = up + jnp.where(first, rim, 0.0)
            if b > 0:
                down = field[b - 1, k, ft, :, rows - RIM :]
                field[b - 1, k, ft, :, rows - RIM :] = down + jnp.where(first, 0.0, rim)
        rims[0, k, ft] = jnp.where(first, rims[blocks - 1, k, ft], rims[0, k, ft])
        return carry

    lax.fori_loop(0, 2 * folds, merge, 0)
    tables = (halves(tab_own[...]), halves(tab_oth[...]))
    sigma = phases[2, 0]

    def transform(load, width, outs):
        x = [
            jnp.concatenate([load(k, c * span, (c + 1) * span) for k in range(2)], axis=1)
            for c in range(radix)
        ]
        if radix == 2:
            turned = sigma * x[1]
            x = [x[0] + turned, x[0] - turned]
        else:
            x = [x[0], x[0]]
        for table, value, out in zip(tables, x, outs):
            y = dot_pieces(table, halves(value))
            out[0] = y[:half, :width] - y[half:, width:]
            out[1] = y[:half, width:] + y[half:, :width]

    def one_block(b, carry):
        load = lambda k, lo, hi: field[b, k, lo:hi].reshape(long, rows)
        transform(load, rows, (own.at[b], oth.at[b]))
        return carry

    lax.fori_loop(0, blocks, one_block, 0)
    pad = jnp.zeros((long, TC - RIM), F32)

    def load_rim(k, lo, hi):
        return jnp.concatenate([rims[0, k, lo:hi].reshape(long, RIM), pad], axis=1)

    transform(load_rim, TC, (own_rim, oth_rim))


def middle_kernel(
    own, own_rim, got, got_rim, spectrum, trig_hi, trig_lo, twist, keep, keep_rim, give, give_rim, mixed
):
    blocks, _, half, rows = own.shape
    groups = RADIX // 2
    per = LONG // rows
    chunks = LONG // TC
    narrow = TC // rows
    lane = lax.broadcasted_iota(jnp.int32, (8, TC), 1)

    def forward(i, carry):
        strip = pl.ds(pl.multiple_of(i * 8, 8), 8)
        for h in range(chunks):
            lanes = slice(h * TC, (h + 1) * TC)

            def fetch(j, k):
                src = own if j < groups else got
                spot = j % groups * per
                if narrow <= 1:
                    return src[spot, k, strip, lanes]
                return jnp.concatenate(
                    [src[spot + h * narrow + u, k, strip, :] for u in range(narrow)], axis=1
                )

            x = [[fetch(j, 0), fetch(j, 1)] for j in range(RADIX)]
            for k in range(2):
                mine, other = own_rim[k, strip, :], got_rim[k, strip, :]
                if h == 0:
                    x[groups][k] = x[groups][k] + jnp.where(lane < RIM // 2, mine, 0.0)
                    x[0][k] = x[0][k] + jnp.where(lane < RIM // 2, other, 0.0)
                if h == chunks - 1:
                    last = lane >= TC - RIM // 2
                    mine = pltpu.roll(mine, TC - RIM, 1)
                    other = pltpu.roll(other, TC - RIM, 1)
                    x[RADIX - 1][k] = x[RADIX - 1][k] + jnp.where(last, mine, 0.0)
                    x[groups - 1][k] = x[groups - 1][k] + jnp.where(last, other, 0.0)
            for d, (re, im) in enumerate(dft8([tuple(v) for v in x], -1.0)):
                c = twist[d : d + 1, lanes]
                s = twist[RADIX + d : RADIX + d + 1, lanes]
                mixed[d, 0, strip, lanes] = re * c - im * s
                mixed[d, 1, strip, lanes] = re * s + im * c
        return carry

    lax.fori_loop(0, half // 8, forward, 0)
    table = (trig_hi[...], trig_lo[...])
    scale = 1.0 / (G * G)
    for d in range(RADIX):
        x = jnp.concatenate([mixed[d, 0], mixed[d, 1]], axis=0)
        y = dot_pieces(halves(x), table)
        factor = spectrum[:, d].reshape(half, LONG) * scale
        re = (y[:half, :LONG] - y[half:, LONG:]) * factor
        im = (y[half:, :LONG] + y[:half, LONG:]) * factor
        y = dot_pieces(halves(jnp.concatenate([re, im], axis=0)), table)
        re = y[:half, :LONG] + y[half:, LONG:]
        im = y[half:, :LONG] - y[:half, LONG:]
        c = twist[d : d + 1, :]
        s = twist[RADIX + d : RADIX + d + 1, :]
        mixed[d, 0] = re * c + im * s
        mixed[d, 1] = im * c - re * s

    def backward(i, carry):
        strip = pl.ds(pl.multiple_of(i * 8, 8), 8)
        edges = {}
        for h in range(chunks):
            lanes = slice(h * TC, (h + 1) * TC)
            x = dft8([(mixed[d, 0, strip, lanes], mixed[d, 1, strip, lanes]) for d in range(RADIX)], 1.0)
            for j in range(RADIX):
                dst = keep if j < groups else give
                spot = j % groups * per
                for k in range(2):
                    if narrow <= 1:
                        dst[spot, k, strip, lanes] = x[j][k]
                    else:
                        for u in range(narrow):
                            dst[spot + h * narrow + u, k, strip, :] = x[j][k][:, u * rows : (u + 1) * rows]
            if h == 0:
                edges[0] = (x[groups], x[0])
            if h == chunks - 1:
                edges[1] = (x[RADIX - 1], x[groups - 1])
        for n, dst in enumerate((keep_rim, give_rim)):
            for k in range(2):
                tail = pltpu.roll(edges[1][n][k], RIM, 1)
                dst[k, strip, :] = jnp.where(lane < RIM // 2, edges[0][n][k], tail)
        return carry

    lax.fori_loop(0, half // 8, backward, 0)


def gather_kernel(
    stat, phases, tab_own, tab_oth, own, own_rim, got, got_rim, out, field, rims
):
    blocks, _, tiles, _ = stat.shape
    _, _, folds, _, rows = field.shape
    ext = rows + RIM
    long = tab_own.shape[0] // 2
    span = long // TC
    radix = folds // span
    tables = (halves(tab_own[...]), halves(tab_oth[...]))
    sigma = phases[2, 0]

    def transform(ins, width, store):
        u = []
        for table, value in zip(tables, ins):
            y = dot_pieces(table, halves(jnp.concatenate([value[0], value[1]], axis=1)))
            u.append((y[:long, :width] + y[long:, width:], y[:long, width:] - y[long:, :width]))
        total = [u[0][k] + u[1][k] for k in range(2)]
        for k in range(2):
            store(k, 0, total[k])
            if radix == 2:
                store(k, 1, sigma * (u[0][k] - u[1][k]))

    def one_block(b, carry):
        def store(k, c, value):
            field[b, k, c * span : (c + 1) * span] = value.reshape(span, TC, rows)

        transform((own.at[b], got.at[b]), rows, store)
        return carry

    lax.fori_loop(0, blocks, one_block, 0)
    first = lax.broadcasted_iota(jnp.int32, (TC, RIM), 1) < RIM // 2

    def store_rim(k, c, value):
        rims[blocks, k, c * span : (c + 1) * span] = value[:, :RIM].reshape(span, TC, RIM)

    transform((own_rim, got_rim), TC, store_rim)

    def near_rows(i, carry):
        k, ft = lax.div(i, folds), lax.rem(i, folds)
        for b in range(blocks):
            up = field[b + 1, k, ft, :, :RIM] if b + 1 < blocks else rims[blocks, k, ft]
            down = field[b - 1, k, ft, :, rows - RIM :] if b > 0 else rims[blocks, k, ft]
            rims[b, k, ft] = jnp.where(first, up, down)
        return carry

    lax.fori_loop(0, 2 * folds, near_rows, 0)

    def one_tile(i, carry):
        b, t = lax.div(i, tiles), lax.rem(i, tiles)
        here = lax.rem(t, folds)
        after, before = lax.rem(t + 1, folds), lax.rem(t + folds - 1, folds)
        slot = [stat[b, j, pl.ds(t, 1), :] for j in range(4)]
        row_tab = stencil_table(slot[0].astype(jnp.int32), slot[2], ext)
        col_tab = stencil_table(slot[1].astype(jnp.int32), slot[3], WIDE)
        part = lax.div(t, span)
        pr, pi = phases[0, part], phases[1, part]
        wr, wi = phases[0, 1], phases[1, 1]
        leave = lax.rem(t + 1, span) == 0
        enter = lax.rem(t, span) == 0
        ar, ai = jnp.where(leave, wr, 1.0), jnp.where(leave, -wi, 0.0)
        br, bi = jnp.where(enter, wr, 1.0), jnp.where(enter, wi, 0.0)

        def whole(k, ft, lo, hi):
            return jnp.concatenate([field[b, k, ft, lo:hi], rims[b, k, ft, lo:hi]], axis=1)

        nr, ni = whole(0, after, 0, RIM), whole(1, after, 0, RIM)
        lr, li = whole(0, before, TC - RIM, TC), whole(1, before, TC - RIM, TC)
        low = lax.broadcasted_iota(jnp.int32, (RIM, ext), 0) < RIM // 2
        edge = (
            jnp.where(low, nr * ar - ni * ai, lr * br - li * bi),
            jnp.where(low, nr * ai + ni * ar, lr * bi + li * br),
        )
        near = jnp.concatenate([whole(0, here, 0, TC), edge[0], whole(1, here, 0, TC), edge[1]], axis=0)
        blended = dot_pieces(halves(near), halves(row_tab))
        vr = jnp.sum(col_tab * blended[:WIDE], axis=0, keepdims=True)
        vi = jnp.sum(col_tab * blended[WIDE:], axis=0, keepdims=True)
        out[b, 0, pl.ds(t, 1), :] = vr * pr + vi * pi
        out[b, 1, pl.ds(t, 1), :] = vi * pr - vr * pi
        return carry

    lax.fori_loop(0, blocks * tiles, one_tile, 0)


def row_sums(values):
    row = lax.broadcasted_iota(jnp.int32, (8, TC), 0)
    tile = jnp.zeros((8, TC), F32)
    for i, value in enumerate(values):
        tile = jnp.where(row == i, value, tile)
    return tile


def full_sum(value):
    return jnp.sum(jnp.sum(value, axis=(0, 1)), keepdims=True).reshape(1, 1)


def update_kernel(
    last, partial, direction, residual, solution, noise, new_direction, new_residual, new_solution,
    parts, mine, got, send_sems, recv_sems, pair_send, pair_recv
):
    at = Place()
    partner = (at.slab, at.rank + 1 - 2 * at.half)
    peers = [
        at.member(at.field, lax.rem(at.own_class + step, at.classes), at.half)
        for step in range(1, at.classes)
    ]
    greet([(d, None) for d in peers] + [(partner, None)], len(peers) + 1)
    copies = []
    for step, device in enumerate(peers, 1):
        copy = remote(partial, parts.at[at.own_class], send_sems.at[step], recv_sems.at[step], device)
        copy.start()
        copies.append(copy)
    parts[at.own_class] = partial[...]
    for copy in copies:
        copy.wait()
    image = parts[0]
    for i in range(1, at.classes):
        image = image + parts[i]
    image = image + noise[0] * direction[...]

    def shared(n, values):
        mine[n] = row_sums(values)
        copy = remote(mine.at[n], got.at[n], pair_send.at[n], pair_recv.at[n], partner)
        copy.start()
        copy.wait()
        return mine[n] + got[n]

    new_residual[...] = image
    sums = []
    for k in range(2):
        sums.append(full_sum(residual[:, k] * residual[:, k]))
    for k in range(2):
        sums.append(full_sum(direction[:, k] * new_residual[:, k]))
    total = shared(0, sums)
    for k in range(2):
        alpha = total[k : k + 1, :1] / total[2 + k : 3 + k, :1]
        new_solution[:, k] = solution[:, k] + alpha * direction[:, k]
        new_residual[:, k] = residual[:, k] - alpha * new_residual[:, k]
    if last:
        new_direction[...] = jnp.zeros_like(new_direction)
        return
    again = shared(1, [full_sum(new_residual[:, k] * new_residual[:, k]) for k in range(2)])
    for k in range(2):
        beta = again[k : k + 1, :1] / total[k : k + 1, :1]
        new_direction[:, k] = new_residual[:, k] + beta * direction[:, k]


def deliver_kernel(solution, residual, out_solution, out_residual, send_sems, recv_sems):
    at = Place()
    goal = (at.half * at.blocks + at.own_class, at.field)
    source = at.member(at.rank, lax.rem(at.slab, at.blocks), lax.div(at.slab, at.blocks))
    same, from_me = at.is_me(*goal), at.is_me(*source)
    barrier = pltpu.get_barrier_semaphore()

    @pl.when(jnp.logical_not(from_me))
    def _():
        pl.semaphore_signal(barrier, inc=1, device_id=source, device_id_type=MESH)

    @pl.when(jnp.logical_not(same))
    def _():
        pl.semaphore_wait(barrier, 1)

    for n, (src, dst) in enumerate(((solution, out_solution), (residual, out_residual))):

        @pl.when(jnp.logical_not(same))
        def _(src=src, dst=dst, n=n):
            remote(src.at[at.own_class], dst, send_sems.at[n], recv_sems.at[n], goal).start()

        @pl.when(same)
        def _(src=src, dst=dst, n=n):
            pltpu.make_async_copy(src.at[at.own_class], dst, recv_sems.at[n]).start()

    for n, (src, dst) in enumerate(((solution, out_solution), (residual, out_residual))):

        @pl.when(jnp.logical_not(same))
        def _(src=src, dst=dst, n=n):
            remote(src.at[at.own_class], dst, send_sems.at[n], recv_sems.at[n], goal).wait()

        @pl.when(same)
        def _(src=src, dst=dst, n=n):
            pltpu.make_async_copy(src.at[at.own_class], dst, recv_sems.at[n]).wait()


def split_table(table):
    high = table.astype(np.float32).astype(BF16)
    low = (table - high.astype(np.float64)).astype(np.float32).astype(BF16)
    return jnp.asarray(high), jnp.asarray(low)


def shape_of(*shape):
    return jax.ShapeDtypeStruct(shape, F32)


def talk(kernel, out_shape, scratch, ident, name, space=pl.ANY, special=()):
    def call(*operands):
        specs = [pl.BlockSpec(memory_space=space)] * len(operands)
        for i in special:
            specs[i] = pl.BlockSpec(memory_space=pltpu.SMEM)
        return pl.pallas_call(
            kernel,
            out_shape=out_shape,
            in_specs=specs,
            out_specs=[pl.BlockSpec(memory_space=space)] * len(out_shape),
            scratch_shapes=scratch,
            compiler_params=pltpu.CompilerParams(collective_id=ident, has_side_effects=True),
            name=name,
        )(*operands)

    return call


def dma(*shape):
    return pltpu.SemaphoreType.DMA(shape)


def per_device(targets, counts, cell_rows, cell_cols, fractions, spectrum, noise_var):
    tiles, capacity = cell_rows.shape
    at = Place()
    slabs, ranks, blocks, classes = at.slabs, at.ranks, at.blocks, at.classes
    rows = G // slabs
    fold = G // classes
    long = min(LONG, fold)
    radix = fold // long
    half = fold // 2
    parts = G // long
    width = spectrum.shape[1]

    slot_index = lax.broadcasted_iota(jnp.int32, (tiles, capacity), 1)
    live = slot_index < counts[:, None]
    stat = jnp.stack(
        [
            jnp.where(live, cell_rows, NOWHERE).astype(F32),
            cell_cols.astype(F32),
            fractions[0],
            fractions[1],
        ]
    )
    targ = jnp.where(live[None], targets, 0.0)

    step = classes if radix == 2 else classes * half
    offsets = [at.own_class + step * at.half, at.own_class + step * (1 - at.half)]
    eighth = jnp.arange(parts, dtype=jnp.int32)
    angle = ((eighth * at.own_class) % parts).astype(F32) * (2.0 * np.pi / parts)
    sigma = jnp.full((parts,), 1.0, F32) * (1.0 - 2.0 * at.half.astype(F32))
    phases = jnp.stack([jnp.cos(angle), -jnp.sin(angle), sigma])
    short = np.arange(long)
    angle = (np.arange(half)[:, None] * short[None, :] % long) * (2.0 * np.pi / long)
    base_cos, base_sin = jnp.asarray(np.cos(angle), F32), jnp.asarray(-np.sin(angle), F32)
    forth, back = [], []
    for offset in offsets:
        angle = ((jnp.arange(long, dtype=jnp.int32) * offset) % G).astype(F32) * (2.0 * np.pi / G)
        c, s = jnp.cos(angle)[None, :], -jnp.sin(angle)[None, :]
        real, imag = base_cos * c - base_sin * s, base_cos * s + base_sin * c
        forth.append(jnp.concatenate([real, imag], axis=0))
        back.append(jnp.concatenate([real.T, imag.T], axis=0))
    short = np.arange(LONG)
    angle = (short[:, None] * short[None, :] % LONG) * (2.0 * np.pi / LONG)
    inner = split_table(np.concatenate([np.cos(angle), -np.sin(angle)], axis=1))
    angle = np.arange(RADIX)[:, None] * short[None, :] * (2.0 * np.pi / G)
    twist = jnp.asarray(np.concatenate([np.cos(angle), -np.sin(angle)], axis=0).astype(np.float32))

    split = radix == 2 and width % (2 * classes * 8) == 0 and classes * 2 == slabs
    out_shape = [shape_of(blocks, 4, tiles, capacity), shape_of(blocks, 2, tiles, capacity)]
    operands = [stat, targ]
    if split:
        kept = width // slabs
        pieces = pl.pallas_call(
            turn_kernel,
            out_shape=shape_of(slabs, RADIX, kept, LONG),
            scratch_shapes=[pltpu.VMEM((LONG // TC, width, TC), F32)],
            name="turn",
        )(spectrum)
        operands.append(pieces)
        out_shape.append(shape_of(slabs, RADIX, kept, LONG))
    sems = [dma(slabs), dma(blocks), dma(classes), dma(blocks), dma(slabs), dma(slabs), dma()]
    collected = talk(
        functools.partial(collect_kernel, split), out_shape, sems, 0, "collect"
    )(*operands)
    if split:
        groups = [[at.deep * i + j for i in range(ranks)] for j in range(at.deep)]
        factors = lax.all_gather(collected[2], "slab", axis_index_groups=groups, axis=0, tiled=True)
        if kept != 8:
            factors = factors.transpose(1, 0, 2, 3).reshape(RADIX, half // 8, 8, LONG)
            factors = factors.transpose(1, 0, 2, 3)
    else:
        everything = lax.all_gather(spectrum, ("slab", "rhs"), axis=1, tiled=True)
        columns = offsets[0] + classes * radix * jnp.arange(half)
        chosen = jnp.take(everything, columns, axis=1).T
        factors = chosen.reshape(half // 8, 8, LONG, RADIX).transpose(0, 3, 1, 2)

    main, rim = shape_of(blocks, 2, half, rows), shape_of(2, half, TC)
    folds = fold // TC
    field = pltpu.VMEM((blocks, 2, folds, TC, rows), F32)
    vmem, smem = pl.BlockSpec(memory_space=pltpu.VMEM), pl.BlockSpec(memory_space=pltpu.SMEM)

    def swap(main_value, rim_value):
        return talk(pair_kernel, [main, rim], [dma(2), dma(2)], 1, "pair")(main_value, rim_value)

    def smoothed(direction):
        own, own_rim, oth, oth_rim = pl.pallas_call(
            spread_kernel,
            out_shape=[main, rim, main, rim],
            in_specs=[vmem, vmem, smem, vmem, vmem],
            scratch_shapes=[field, pltpu.VMEM((blocks, 2, folds, TC, RIM), F32)],
            name="spread",
        )(collected[0], direction, phases, *forth)
        got, got_rim = swap(oth, oth_rim)
        keep, keep_rim, give, give_rim = pl.pallas_call(
            middle_kernel,
            out_shape=[main, rim, main, rim],
            scratch_shapes=[pltpu.VMEM((RADIX, 2, half, LONG), F32)],
            name="middle",
        )(own, own_rim, got, got_rim, factors, *inner, twist)
        got, got_rim = swap(give, give_rim)
        return pl.pallas_call(
            gather_kernel,
            out_shape=shape_of(*direction.shape),
            in_specs=[vmem, smem] + [vmem] * 6,
            scratch_shapes=[field, pltpu.VMEM((blocks + 1, 2, folds, TC, RIM), F32)],
            name="gather",
        )(collected[0], phases, *back, keep, keep_rim, got, got_rim)

    residual = collected[1]
    solution = jnp.zeros(residual.shape, F32)
    direction = residual
    points = shape_of(*residual.shape)
    for repeat in range(ITERS):
        last = repeat + 1 == ITERS
        direction, residual, solution = talk(
            functools.partial(update_kernel, last),
            [points] * 3,
            [
                pltpu.VMEM((classes, *residual.shape), F32),
                pltpu.VMEM((2, 8, TC), F32),
                pltpu.VMEM((2, 8, TC), F32),
                dma(classes),
                dma(classes),
                dma(2),
                dma(2),
            ],
            2 + last,
            "update",
            pltpu.VMEM,
            (4,),
        )(smoothed(direction), direction, residual, solution, noise_var)
    out = shape_of(2, tiles, capacity)
    solution, residual = talk(deliver_kernel, [out, out], [dma(2), dma(2)], 4, "deliver")(
        solution, residual
    )
    return (solution, residual)


def solution(mesh):
    placed = (
        P("rhs", "slab", None),
        P("slab"),
        P("slab", None),
        P("slab", None),
        P(None, "slab", None),
        P(None, ("slab", "rhs")),
        P(),
    )
    return jax.shard_map(
        per_device,
        mesh=mesh,
        in_specs=placed,
        out_specs=(P("rhs", "slab", None), P("rhs", "slab", None)),
        check_vma=False,
    )
```
